64 devices in a mesh: batch: 4 (over x, y), t: 16 (over z, core).
Axes of the slice: x: 2, y: 2, z: 8, core: 2. Of those that a mesh axis runs over, the one named last changes fastest.
The devices are a block of a 4x4x8 slice.
Arguments:
- z: bfloat16 [128, 12, 24, 256], P(('batch', 't')), parts along dimension 0
- w: bfloat16 [5, 3, 3, 3, 256, 256], replicated
- b: float32 [5, 256], replicated
- gamma: float32 [4, 256], replicated
- beta: float32 [4, 256], replicated
Outputs:
- output: bfloat16 [256, 24, 48, 256], P(('batch', 't')), parts along dimension 0
There are 4 independent parts. The reference program is written for one: setup_inputs(seed, part) draws one part's arguments, and reference() takes and returns one part's arrays. A program takes and returns all parts, laid end to end along the dimension named above; an argument that names none is the same for every part.
All inputs are finite; a program needn't handle non-finite values.
Results may differ from the reference program's by a relative error of at most 0.0144827.
Values are sent between devices in bfloat16 or wider.
A program may use at most 768 MiB of HBM per device.

```python
import jax
import jax.numpy as jnp
from jax import lax

T = 32
H = 12
W = 24
C = 256
GROUPS = 32
EPS = 1e-6
DN = ('NDHWC', 'DHWIO', 'NDHWC')


def setup_inputs(seed: int = 0, part: int = 0) -> dict:
    key = jax.random.key(seed)
    kz, ka, km = jax.random.split(jax.random.fold_in(key, part), 3)
    kw, kb, kg, kbe = jax.random.split(key, 4)
    amp = jnp.exp(0.5 * jax.random.normal(ka, (T, 1, 1, 1), jnp.float32))
    ramp = jnp.linspace(-1.0, 1.0, T)[:, None, None, None]
    mean = ramp * jax.random.normal(km, (1, 1, 1, C), jnp.float32)
    z = amp * jax.random.normal(kz, (T, H, W, C), jnp.float32) + mean
    w = jax.random.normal(kw, (5, 3, 3, 3, C, C), jnp.float32) * (27 * C) ** -0.5
    b = 0.1 * jax.random.normal(kb, (5, C), jnp.float32)
    gamma = 1.0 + 0.2 * jax.random.normal(kg, (4, C), jnp.float32)
    beta = 0.2 * jax.random.normal(kbe, (4, C), jnp.float32)
    return {'z': z.astype(jnp.bfloat16), 'w': w.astype(jnp.bfloat16), 'b': b, 'gamma': gamma, 'beta': beta}


def _conv(x, wk, bk):
    xp = jnp.concatenate([x[:1], x[:1], x], axis=0).astype(jnp.float32)
    y = lax.conv_general_dilated(xp[None], wk.astype(jnp.float32), (1, 1, 1), ((0, 0), (1, 1), (1, 1)), dimension_numbers=DN)[0]
    return (y + bk).astype(jnp.bfloat16)


def _norm_act(x, g, be):
    xf = x.astype(jnp.float32).reshape(x.shape[:-1] + (GROUPS, x.shape[-1] // GROUPS))
    cnt = xf.size // GROUPS
    mean = jnp.sum(xf, axis=(0, 1, 2, 4)) / cnt
    var = jnp.sum(xf * xf, axis=(0, 1, 2, 4)) / cnt - mean * mean
    xn = ((xf - mean[:, None]) * lax.rsqrt(var + EPS)[:, None]).reshape(x.shape) * g + be
    xn = xn.astype(jnp.bfloat16).astype(jnp.float32)
    return jax.nn.silu(xn).astype(jnp.bfloat16)


def _resblock(x, w, b, gamma, beta, i, j):
    h = _conv(_norm_act(x, gamma[i], beta[i]), w[j], b[j])
    h = _conv(_norm_act(h, gamma[i + 1], beta[i + 1]), w[j + 1], b[j + 1])
    return (x.astype(jnp.float32) + h.astype(jnp.float32)).astype(jnp.bfloat16)


def _upsample(x):
    x = jnp.repeat(jnp.repeat(x, 2, axis=1), 2, axis=2)
    return jnp.concatenate([x[:1], jnp.repeat(x[1:], 2, axis=0)], axis=0)


def reference(z, w, b, gamma, beta):
    x = _resblock(z, w, b, gamma, beta, 0, 0)
    u = _conv(_upsample(x), w[2], b[2])
    y = _resblock(u, w, b, gamma, beta, 2, 3)
    return jnp.concatenate([y[:1], y], axis=0)
```

```python
import functools

import jax
import jax.numpy as jnp
from jax import lax
from jax.experimental import pallas as pl
from jax.experimental.pallas import tpu as pltpu
from jax.sharding import PartitionSpec as P

GROUPS = 32
EPS = 1e-6
MESH = pl.DeviceIdType.MESH
BF = jnp.bfloat16
F32 = jnp.float32


def partial_sums(v):
    r = v.reshape(v.shape[0] // 8, 8, v.shape[1])
    return jnp.sum(r, axis=0), jnp.sum(r * r, axis=0)


def shifted(v, width):
    n = v.shape[0]
    col = lax.broadcasted_iota(jnp.int32, v.shape, 0) % width
    before = jnp.where(col == 0, 0.0, pltpu.roll(v, 1, 0))
    after = jnp.where(col == width - 1, 0.0, pltpu.roll(v, n - 1, 0))
    return before, v, after


def activate(v, mean, a, be):
    t = ((v.astype(F32) - mean) * a + be).astype(BF).astype(F32) * 0.5
    return t + t * jnp.tanh(t)


def kernel(nt, n, hh, ww, z_hbm, w_hbm, b_ref, gamma_ref, beta_ref, y_hbm,
           W, Z, H1, X, U, H3, Y, A0, A1, AB, PP, U32, G, BD, wsem, zsem, ysem, ssem, rsem):
    me = lax.axis_index('t')
    c = z_hbm.shape[-1]
    m1, m2 = hh * ww, 4 * hh * ww
    h2, w2 = 2 * hh, 2 * ww
    n2 = 2 * n
    first = me == 0

    def peer(d):
        return {'t': lax.rem(me + d, nt)}

    barrier = pltpu.get_barrier_semaphore()
    for d in range(1, nt):
        pl.semaphore_signal(barrier, inc=1, device_id=peer(d), device_id_type=MESH)
    zcopy = pltpu.make_async_copy(z_hbm, Z.at[pl.ds(2, n)], zsem)
    zcopy.start()
    wcopies = [pltpu.make_async_copy(w_hbm.at[i], W.at[i], wsem.at[i]) for i in range(5)]
    for copy in wcopies:
        copy.start()

    zero_row = jnp.zeros((w2, 3 * c), BF)
    for f in range(n2 + 2):
        AB[f, 0] = zero_row
        AB[f, h2 + 1] = zero_row
    gi = lax.broadcasted_iota(jnp.int32, (c, c), 0) // (c // GROUPS)
    gj = lax.broadcasted_iota(jnp.int32, (c, c), 1) // (c // GROUPS)
    BD[...] = jnp.where(gi == gj, 1.0, 0.0).astype(F32)

    def stat_copy(i, d):
        return pltpu.make_async_remote_copy(
            src_ref=G.at[i, 0], dst_ref=G.at[i, d], send_sem=ssem.at[i, d], recv_sem=rsem.at[i, d],
            device_id=peer(d), device_id_type=MESH)

    def send_stats(i, s1, s2):
        G[i, 0, 0:1, :] = jnp.sum(s1, axis=0, keepdims=True)
        G[i, 0, 1:2, :] = jnp.sum(s2, axis=0, keepdims=True)
        for d in range(nt // 2, 0, -1):
            stat_copy(i, d).start()
            if d != nt - d:
                stat_copy(i, nt - d).start()

    def norm(i, cnt):
        for d in range(1, nt):
            stat_copy(i, d).wait()
        tot = jnp.sum(G[i], axis=0)
        tot = jnp.dot(tot, BD[...], precision=lax.Precision.HIGHEST, preferred_element_type=F32)
        mean = tot[0:1] / cnt
        var = tot[1:2] / cnt - mean * mean
        return mean, lax.rsqrt(var + EPS) * gamma_ref[i:i + 1, :], beta_ref[i:i + 1, :]

    def halo(k, buf, src, dst, count):
        return pltpu.make_async_remote_copy(
            src_ref=buf.at[pl.ds(src, count)], dst_ref=buf.at[pl.ds(dst, count)],
            send_sem=ssem.at[4, k], recv_sem=rsem.at[4, k], device_id=peer(1), device_id_type=MESH)

    cnt1 = float(nt * n * m1 * (c // GROUPS))
    zcopy.wait()
    s1, s2 = partial_sums(Z[pl.ds(2, n)].reshape(n * m1, c).astype(F32))
    pl.semaphore_wait(barrier, nt - 1)
    send_stats(0, s1, s2)
    hz = halo(0, Z, n, 0, 2)
    hz.start()

    def fill_a(src, i, mean, a, be):
        pad = jnp.zeros((ww, c), F32)

        def body(f, _):
            v = src[f]
            own = src[2]
            v = jnp.where(jnp.logical_and(first, f < 2), own.astype(F32), v.astype(F32))
            act = activate(v, mean, a, be)
            for dj, s in enumerate(shifted(act, ww)):
                A0[f, :, dj * c:(dj + 1) * c] = s.astype(BF)
                A1[f, :, dj * c:(dj + 1) * c] = jnp.concatenate([pad, s, pad], axis=0).astype(BF)
            return 0

        lax.fori_loop(0, n + 2, body, 0)

    def conv_a(j):
        acc = None
        for k in range(3):
            for di in range(3):
                lhs = A0[k:k + n] if di == 1 else A1[k:k + n, di * ww:di * ww + m1]
                d = jnp.dot(lhs.reshape(n * m1, 3 * c), W[j, 3 * k + di], preferred_element_type=F32)
                acc = d if acc is None else acc + d
        return (acc + b_ref[j:j + 1, :]).astype(BF)

    mean, a, be = norm(0, cnt1)
    hz.wait()
    fill_a(Z, 0, mean, a, be)
    wcopies[0].wait()
    h = conv_a(0)
    H1[pl.ds(2, n)] = h.reshape(n, m1, c)
    s1, s2 = partial_sums(h.astype(F32))
    send_stats(1, s1, s2)
    hh1 = halo(1, H1, n, 0, 2)
    hh1.start()
    mean, a, be = norm(1, cnt1)
    hh1.wait()
    fill_a(H1, 1, mean, a, be)
    wcopies[1].wait()
    h = conv_a(1).astype(F32)
    X[pl.ds(1, n)] = (Z[pl.ds(2, n)].reshape(n * m1, c).astype(F32) + h).astype(BF).reshape(n, m1, c)
    hx = halo(2, X, n, 0, 1)
    hx.start()

    wcopies[2].wait()
    zeros8 = jnp.zeros((8, c), F32)
    edge = lax.broadcasted_iota(jnp.int32, (ww, c), 0)
    bias2 = b_ref[2:3, :]

    def up(jj, carry):
        j = n - 1 - jj

        @pl.when(jj == n - 1)
        def _():
            hx.wait()

            @pl.when(first)
            def _():
                X[0] = X[1]

        for di in range(3):
            for dj in range(3):
                def tap(k):
                    return W[2, 3 * k + di, dj * c:(dj + 1) * c, :]

                s = jnp.dot(X[j + 1], tap(2), preferred_element_type=F32) + jnp.dot(X[j], tap(0), preferred_element_type=F32)
                mid = jnp.dot(X[pl.ds(j, 2)].reshape(2 * m1, c), tap(1), preferred_element_type=F32)
                PP[0, 3 * di + dj] = s + mid[:m1]
                PP[1, 3 * di + dj] = s + mid[m1:]

        def spread(e, carry):
            s1, s2 = carry
            cache = {}

            def cols(di, i):
                if i < 0 or i >= hh:
                    return None
                if (di, i) not in cache:
                    left, mid, right = (PP[e, 3 * di + dj, i * ww:(i + 1) * ww] for dj in range(3))
                    even = jnp.where(edge == 0, 0.0, pltpu.roll(left, 1, 0)) + mid + right
                    odd = left + mid + jnp.where(edge == ww - 1, 0.0, pltpu.roll(right, ww - 1, 0))
                    cache[di, i] = (even, odd)
                return cache[di, i]

            t1, t2 = zeros8, zeros8
            for i in range(hh):
                for r, parts in enumerate(((cols(0, i - 1), cols(1, i), cols(2, i)), (cols(0, i), cols(1, i), cols(2, i + 1)))):
                    for s in range(2):
                        v = bias2
                        for part in parts:
                            if part is not None:
                                v = part[s] + v
                        v = v.astype(BF).astype(F32)
                        p1, p2 = partial_sums(v)
                        t1, t2 = t1 + p1, t2 + p2
                        for q in range(c // 128):
                            U32[q, 2 * i + r, pl.ds(s, ww, stride=2), :] = v[:, q * 128:(q + 1) * 128]
            pos = 2 * j + e
            for i in range(0, h2, 2):
                for q in range(c // 128):
                    U[pos + 2, i * w2:(i + 2) * w2, q * 128:(q + 1) * 128] = U32[q, i:i + 2].reshape(2 * w2, 128).astype(BF)
            wt = jnp.where(jnp.logical_and(first, pos == 0), 0.0, 1.0)
            return s1 + wt * t1, s2 + wt * t2

        return lax.fori_loop(0, 2, spread, carry)

    s1, s2 = lax.fori_loop(0, n, up, (zeros8, zeros8))

    cnt2 = float((nt * n2 - 1) * m2 * (c // GROUPS))
    send_stats(2, s1, s2)
    hu = [halo(3, U, n2 + 1, 1, 1), halo(4, U, n2, 0, 1)]
    for copy in hu:
        copy.start()

    def fill_b(src, f, mean, a, be):
        rows = 2 * w2
        for i in range(0, h2, 2):
            act = activate(src[f, i * w2:i * w2 + rows], mean, a, be)
            for dj, s in enumerate(shifted(act, w2)):
                AB[f, i + 1:i + 3, :, dj * c:(dj + 1) * c] = s.astype(BF).reshape(2, w2, c)

    def conv_b(src, j, mean, a, be, copies, finish, carry):
        lax.fori_loop(2, n2 + 2, lambda f, _: (fill_b(src, f, mean, a, be), 0)[1], 0)
        half = h2 // 2

        def body(k, carry):
            f = n2 - 1 - k

            @pl.when(f == 1)
            def _():
                for copy in copies:
                    copy.wait()

                @pl.when(first)
                def _():
                    for s in range(2):
                        src[s] = src[2]

                lax.fori_loop(0, 2, lambda g, _: (fill_b(src, g, mean, a, be), 0)[1], 0)

            for q in range(2):
                acc = None
                for t in range(9):
                    lhs = AB[f + t // 3, q * half + t % 3:q * half + t % 3 + half]
                    d = jnp.dot(lhs.reshape(half * w2, 3 * c), W[j, t], preferred_element_type=F32)
                    acc = d if acc is None else acc + d
                carry = finish(f, q * half * w2, half * w2, (acc + b_ref[j:j + 1, :]).astype(BF), carry)
            return carry

        return lax.fori_loop(0, n2, body, carry)

    mean, a, be = norm(2, cnt2)
    wcopies[3].wait()
    hh3 = [halo(5, H3, n2 + 1, 1, 1), halo(6, H3, n2, 0, 1)]

    def finish3(f, row, rows, h, carry):
        H3[f + 2, row:row + rows] = h
        if row > 0:
            for g, copy in ((n2 - 1, hh3[0]), (n2 - 2, hh3[1])):
                pl.when(f == g)(copy.start)
        t1, t2 = partial_sums(h.astype(F32))
        wt = jnp.where(jnp.logical_and(first, f == 0), 0.0, 1.0)
        return carry[0] + wt * t1, carry[1] + wt * t2

    s1, s2 = conv_b(U, 3, mean, a, be, hu, finish3, (zeros8, zeros8))
    send_stats(3, s1, s2)
    mean, a, be = norm(3, cnt2)
    wcopies[4].wait()

    def ycopy(f):
        return pltpu.make_async_copy(Y.at[f], y_hbm.at[f], ysem.at[f])

    def finish4(f, row, rows, h, carry):
        Y[f, row:row + rows] = (U[f + 2, row:row + rows].astype(F32) + h.astype(F32)).astype(BF)
        if row > 0:
            ycopy(f).start()
        return carry

    conv_b(H3, 4, mean, a, be, hh3, finish4, 0)
    for f in range(n2):
        ycopy(f).wait()


def solution(mesh):
    nt = mesh.shape['t']

    def local(z, w, b, gamma, beta):
        n, hh, ww, c = z.shape
        m1, m2, n2 = hh * ww, 4 * hh * ww, 2 * n
        vmem = pl.BlockSpec(memory_space=pltpu.VMEM)
        hbm = pl.BlockSpec(memory_space=pl.ANY)
        y = pl.pallas_call(
            functools.partial(kernel, nt, n, hh, ww),
            out_shape=jax.ShapeDtypeStruct((n2, m2, c), BF),
            in_specs=[hbm, hbm, vmem, vmem, vmem],
            out_specs=hbm,
            scratch_shapes=[
                pltpu.VMEM((5, 9, 3 * c, c), BF),
                pltpu.VMEM((n + 2, m1, c), BF),
                pltpu.VMEM((n + 2, m1, c), BF),
                pltpu.VMEM((n + 1, m1, c), BF),
                pltpu.VMEM((n2 + 2, m2, c), BF),
                pltpu.VMEM((n2 + 2, m2, c), BF),
                pltpu.VMEM((n2, m2, c), BF),
                pltpu.VMEM((n + 2, m1, 3 * c), BF),
                pltpu.VMEM((n + 2, m1 + 2 * ww, 3 * c), BF),
                pltpu.VMEM((n2 + 2, 2 * hh + 2, 2 * ww, 3 * c), BF),
                pltpu.VMEM((2, 9, m1, c), F32),
                pltpu.VMEM((c // 128, 2 * hh, 2 * ww, 128), F32),
                pltpu.VMEM((4, nt, 2, c), F32),
                pltpu.VMEM((c, c), F32),
                pltpu.SemaphoreType.DMA((5,)),
                pltpu.SemaphoreType.DMA,
                pltpu.SemaphoreType.DMA((n2,)),
                pltpu.SemaphoreType.DMA((5, max(nt, 7))),
                pltpu.SemaphoreType.DMA((5, max(nt, 7))),
            ],
            compiler_params=pltpu.CompilerParams(
                collective_id=0, has_side_effects=True, vmem_limit_bytes=67_043_328),
            name='vae_up_block',
        )(z.reshape(n, m1, c), w.reshape(5, 9, 3 * c, c), b, gamma, beta)
        return y.reshape(n2, 2 * hh, 2 * ww, c)

    spec = P(('batch', 't'))
    return jax.shard_map(local, mesh=mesh, in_specs=(spec, P(), P(), P(), P()), out_specs=spec, check_vma=False)
```
